32 devices in a mesh: child: 4 (over z), rows: 8 (over y, x, core).
Axes of the slice: x: 2, y: 2, z: 4, core: 2. Of those that a mesh axis runs over, the one named last changes fastest.
Arguments:
- omega: bfloat16 [4, 8192, 512], P('child', 'rows'), may hold values from -6 to 6
- leaf_diag: bfloat16 [4, 32, 256, 256], P('child', 'rows'), may hold values from -0.375 to 0.375
- leaf_u: bfloat16 [4, 8192, 128], P('child', 'rows'), may hold values from -0.5 to 0.5
- leaf_v: bfloat16 [4, 8192, 128], P('child', 'rows'), may hold values from -0.375 to 0.375
- coupling: bfloat16 [4, 4096, 4096], P('child', 'rows'), may hold values from -0.09375 to 0.09375
- child_map: int32 [4, 64], P('child', 'rows'), may hold values from 0 to 95, as said below
Outputs:
- parent_rows: float32 [3, 4096, 512], P(None, ('child', 'rows'))
The draws below stay inside these ranges and needn't reach their ends.
Inputs may be any that keep to these rules, and one draw needn't show every extreme that they name: `child_map`: child block b of every child maps to one of the parent blocks 3 * (b // 2), 3 * (b // 2) + 1, 3 * (b // 2) + 2, and blocks 2 k and 2 k + 1 map to two different ones of their triple, the lower first.
All inputs are finite; a program needn't handle non-finite values.
Results may differ from the reference program's by a relative error of at most 0.004.
Values may be sent and summed in bfloat16 or wider, within the bound.
No kernel may reach another device: no remote copies, remote signals or barrier semaphores. Data moves between devices by JAX's collectives and lax.ppermute only.
A program may use at most 128 MiB of HBM per device.

```python
import jax
import jax.numpy as jnp
from jax import lax

L = 256
R = 128
S = 512
LEAF_DEV = 4
NLEAF = 32
NC = 8192
NCB = 64
PBLK_DEV = 3
N_CHILD = 4
N_ROWS = 8


def draw_child_map(key, part):
    pairs = NCB // 2
    omitted = jax.random.randint(key, (N_CHILD, pairs), 0, 3)
    first = jnp.where(omitted == 0, 1, 0)
    second = jnp.where(omitted == 2, 1, 2)
    triple = 3 * jnp.arange(pairs, dtype=jnp.int32)[None, :]
    both = jnp.stack([triple + first, triple + second], axis=2)
    return both.reshape(N_CHILD, NCB).astype(jnp.int32)


def levels(stream_key, dims, split, least, largest):
    def one(position, shards_of):
        steps = jax.random.uniform(jax.random.fold_in(jax.random.fold_in(stream_key, 6), position), (shards_of,), jnp.float32, least / len(split), largest / len(split))
        return jnp.repeat(jnp.exp(steps), dims[position] // shards_of).reshape((-1,) + (1,) * (len(dims) - position - 1))

    gain = one(*split[0])
    for cut in split[1:]:
        gain = gain * one(*cut)
    return gain


def bell_draw(key, extent, scale, reach, pieces=(), kind=jnp.bfloat16):
    result = scale * jax.random.normal(key, extent, jnp.float32)
    if pieces:
        result = result * levels(key, extent, pieces, -0.22, 0.18)
    return jnp.clip(result, -reach, reach).astype(kind)


def setup_inputs(seed: int = 0) -> dict:
    seeds = jax.random.split(jax.random.key(seed), 7)
    return {
        "omega": bell_draw(seeds[0], (N_CHILD, NC, S), 1.0, 6.0, ((0, 4), (1, 8))),
        "leaf_diag": bell_draw(seeds[1], (N_CHILD, NLEAF, L, L), L ** -0.5, 0.375, ((0, 4), (1, 8))),
        "leaf_u": bell_draw(seeds[2], (N_CHILD, NC, R), R ** -0.5, 0.5, ((0, 4), (1, 8))),
        "leaf_v": bell_draw(seeds[3], (N_CHILD, NC, R), L ** -0.5, 0.375, ((0, 4), (1, 8))),
        "coupling": bell_draw(seeds[4], (N_CHILD, NLEAF * R, NLEAF * R), (NLEAF * R) ** -0.5, 0.09375, ((0, 4), (1, 8))),
        "child_map": draw_child_map(jax.random.fold_in(seeds[6], 71), 0),
    }


def reference(omega, leaf_diag, leaf_u, leaf_v, coupling, child_map):
    block_rows = L // 2
    parent_count = 3 * LEAF_DEV * N_ROWS
    parent = jnp.zeros((parent_count, block_rows, S), jnp.float32)
    for child_index in range(N_CHILD):
        omega_leaves = omega[child_index].astype(jnp.float32).reshape(NLEAF, L, S)
        basis_in = leaf_v[child_index].astype(jnp.float32).reshape(NLEAF, L, R)
        basis_out = leaf_u[child_index].astype(jnp.float32).reshape(NLEAF, L, R)
        sampled = jnp.einsum("nlr,nls->nrs", basis_in, omega_leaves).astype(jnp.bfloat16).reshape(NLEAF * R, S)
        coupled = jnp.dot(coupling[child_index], sampled, preferred_element_type=jnp.float32).astype(jnp.bfloat16)
        coupled = lax.optimization_barrier(coupled).astype(jnp.float32).reshape(NLEAF, R, S)
        local_part = jnp.einsum("nij,njs->nis", leaf_diag[child_index].astype(jnp.float32), omega_leaves)
        local_part = local_part + jnp.einsum("nlr,nrs->nls", basis_out, coupled)
        update = lax.optimization_barrier(local_part.astype(jnp.bfloat16)).astype(jnp.float32)
        update = update.reshape(2 * NLEAF, block_rows, S)
        parent = parent.at[child_map[child_index].astype(jnp.int32)].add(update)
    parent = parent.reshape(N_ROWS, N_CHILD, PBLK_DEV, block_rows, S)
    parent = jnp.transpose(parent, (2, 1, 0, 3, 4))
    return parent.reshape(PBLK_DEV, N_CHILD * N_ROWS * block_rows, S)
```

```python
import jax
import jax.numpy as jnp
from jax import lax
from jax.sharding import PartitionSpec as P

CHUNKS = 1


def on_device(omega, leaf_diag, leaf_u, leaf_v, coupling, child_map):
    leaves = leaf_diag.shape[1]
    leaf_size = leaf_diag.shape[2]
    leaf_rank = leaf_u.shape[2]
    samples = omega.shape[2]
    block_rows = leaf_size // 2
    n_rows = lax.axis_size("rows")
    n_child = lax.axis_size("child")
    r = lax.axis_index("rows")
    c = lax.axis_index("child")
    own_rows = leaves * leaf_rank
    half = own_rows // 2
    group = leaves // n_child
    width = samples // CHUNKS

    def swap_rows(value, mask):
        return lax.ppermute(value, "rows", [(i, i ^ mask) for i in range(n_rows)])

    def shift_child(value, d):
        return lax.ppermute(value, "child", [(i, (i + d) % n_child) for i in range(n_child)])

    omega_leaves = omega[0].reshape(leaves, leaf_size, samples)
    basis_in = leaf_v[0].reshape(leaves, leaf_size, leaf_rank)
    basis_out = leaf_u[0].reshape(leaves, leaf_size, leaf_rank)
    coupling_rows = coupling[0]

    maps = [child_map[0]] + [shift_child(child_map[0], d) for d in range(1, n_child)]
    slots = 3 * group
    base = 3 * leaves * r + slots * c
    slot_of = []
    for d in range(n_child):
        mine = lax.dynamic_slice(maps[d], (2 * group * c,), (2 * group,))
        slot_of.append(mine - base)

    out = []
    for k in range(CHUNKS):
        cols = omega_leaves[:, :, k * width : (k + 1) * width]
        sampled = jnp.einsum("nlr,nls->nrs", basis_in, cols, preferred_element_type=jnp.float32)
        sampled = sampled.astype(jnp.bfloat16).reshape(own_rows, width)
        pieces = {0: [(0, sampled)]}
        for m in range(2, n_rows, 2):
            if m & (m - 1) == 0:
                pieces[m] = [(0, swap_rows(sampled, m))]
        ends = {m: (v[0][1][:half], v[0][1][half:]) for m, v in pieces.items()}
        for m in range(2, n_rows, 2):
            if m & (m - 1):
                high = 1 << (m.bit_length() - 1)
                low = m & -m
                first = swap_rows(ends[m ^ high][0], high)
                second = swap_rows(ends[m ^ low][1], low)
                ends[m] = (first, second)
                pieces[m] = [(0, first), (half, second)]
        for m in range(0, n_rows, 2):
            pieces[m ^ 1] = [(at, swap_rows(v, 1)) for at, v in pieces[m]]
        acc = None
        for m in sorted(pieces, key=lambda m: (bin(m >> 1).count("1"), m)):
            for at, v in pieces[m]:
                weights = lax.dynamic_slice(
                    coupling_rows, (0, (r ^ m) * own_rows + at), (own_rows, v.shape[0])
                )
                part = jnp.dot(weights, v, preferred_element_type=jnp.float32)
                acc = part if acc is None else acc + part
        coupled = acc.astype(jnp.bfloat16)
        local_part = jnp.einsum("nij,njs->nis", leaf_diag[0], cols, preferred_element_type=jnp.float32)
        local_part = local_part + jnp.einsum(
            "nlr,nrs->nls",
            basis_out,
            coupled.reshape(leaves, leaf_rank, width),
            preferred_element_type=jnp.float32,
        )
        update = local_part.astype(jnp.bfloat16).reshape(2 * leaves, block_rows, width)
        arrived = []
        for d in range(n_child):
            to = (c + d) % n_child
            sent = lax.dynamic_slice(
                update, (2 * group * to, 0, 0), (2 * group, block_rows, width)
            )
            arrived.append(shift_child(sent, d) if d else sent)
        rows = []
        for s in range(slots):
            total = jnp.zeros((block_rows, width), jnp.float32)
            leaf = s // 3
            for d in range(n_child):
                for b in (2 * leaf, 2 * leaf + 1):
                    block = arrived[d][b].astype(jnp.float32)
                    total = total + jnp.where(slot_of[d][b] == s, block, 0.0)
            rows.append(total)
        out.append(jnp.stack(rows))
    return jnp.concatenate(out, axis=2)


def solution(mesh):
    placed = (
        P("child", "rows", None),
        P("child", "rows", None, None),
        P("child", "rows", None),
        P("child", "rows", None),
        P("child", "rows", None),
        P("child", "rows"),
    )
    return jax.shard_map(
        on_device,
        mesh=mesh,
        in_specs=placed,
        out_specs=P(None, ("child", "rows"), None),
        check_vma=False,
    )
```
